32 devices in a mesh: dp: 2 (over x), section: 4 (over y, core), tensor: 4 (over z).
Axes of the slice: x: 2, y: 2, z: 4, core: 2. Of those that a mesh axis runs over, the one named last changes fastest.
Arguments:
- failed_section: int32 [2], P('dp'), may hold values from 0 to 999
- token_ids: int32 [2, 2048], P('dp'), may hold values from 0 to 100001, as said below
- section_outputs: bfloat16 [2, 4, 2048, 2048], P('dp', 'section', None, 'tensor'), may hold values from -11 to 11
- w_query: float32 [4, 2048, 1024], P('section', 'dp', 'tensor'), may hold values from -1 to 1
- w_key: float32 [4, 2048, 1024], P('section', 'dp', 'tensor'), may hold values from -2 to 2
- w_value: float32 [4, 2048, 1024], P('section', 'dp', 'tensor'), may hold values from -0.125 to 0.125
- w_out: float32 [4, 2048, 1024], P('section', 'dp', 'tensor'), may hold values from -0.75 to 0.75
- m_value: float32 [4, 2048, 1024], P('section', 'dp', 'tensor'), may hold values from -3 to 3
- v_value: float32 [4, 2048, 1024], P('section', 'dp', 'tensor'), may hold values from 0.001 to 1
- m_out: float32 [4, 2048, 1024], P('section', 'dp', 'tensor'), may hold values from -3 to 3
- v_out: float32 [4, 2048, 1024], P('section', 'dp', 'tensor'), may hold values from 0.001 to 1
Outputs:
- restored_query: float32 [2, 4, 2048, 1024], P('dp', 'section', None, 'tensor')
- restored_key: float32 [2, 4, 2048, 1024], P('dp', 'section', None, 'tensor')
- restored_value: float32 [2, 4, 2048, 1024], P('dp', 'section', None, 'tensor')
- restored_out: float32 [2, 4, 2048, 1024], P('dp', 'section', None, 'tensor')
- restored_m_value: float32 [2, 4, 2048, 1024], P('dp', 'section', None, 'tensor')
- restored_v_value: float32 [2, 4, 2048, 1024], P('dp', 'section', None, 'tensor')
- restored_m_out: float32 [2, 4, 2048, 1024], P('dp', 'section', None, 'tensor')
- restored_v_out: float32 [2, 4, 2048, 1024], P('dp', 'section', None, 'tensor')
- attn_update: bfloat16 [2, 4, 2048, 2048], P('dp', 'section', None, 'tensor')
The draws below stay inside these ranges and needn't reach their ends.
Inputs may be any that keep to these rules, and one draw needn't show every extreme that they name: `token_ids`: token ids of each replica's micro-batch; the id 100001 ends a document, the others are ordinary tokens below 100000.
All inputs are finite; a program needn't handle non-finite values.
Results may differ from the reference program's by a relative error of at most 0.0087.
Values may be sent and summed in bfloat16 or wider, within the bound.
A program may use at most 128 MiB of HBM per device.

```python
import math
import jax
import jax.numpy as jnp
from jax import lax

D = 2048
HD = 128
HEADS = 8
TOKENS = 2048
INNER = 1024
REPLICAS = 2
SECTIONS = 4


def draw_token_ids(key, part):
    word_ids = jax.random.randint(jax.random.fold_in(key, 11), (REPLICAS, TOKENS), 0, 100000)
    doc_marks = jax.random.randint(jax.random.fold_in(key, 12), (REPLICAS, TOKENS), 0, max(2, TOKENS // 8))
    return jnp.where(doc_marks == 0, 100001, word_ids).astype(jnp.int32)


def draw_section_outputs(key, part):
    full_shape = (REPLICAS, SECTIONS, TOKENS, D)
    entries = jnp.clip(jax.random.normal(jax.random.fold_in(key, 23), full_shape, jnp.float32), -6.0, 6.0)
    return entries.astype(jnp.bfloat16)


def projection_pair(key):
    full_shape = (SECTIONS, D, INNER)
    leading = jnp.clip(jax.random.normal(jax.random.fold_in(key, 31), full_shape, jnp.float32), -6.0, 6.0) / math.sqrt(D)
    other = jnp.clip(jax.random.normal(jax.random.fold_in(key, 32), full_shape, jnp.float32), -6.0, 6.0) / math.sqrt(D)
    second = other
    return (leading, second)


def draw_w_query(key, part):
    return projection_pair(key)[0].astype(jnp.float32)


def draw_w_key(key, part):
    return projection_pair(key)[1].astype(jnp.float32)


def block_levels(rng, dims, pieces, least, top_value):
    level, own = 1.0, jax.random.fold_in(rng, 6)
    for dim, parts in pieces:
        draws = jnp.exp(jax.random.uniform(jax.random.fold_in(own, dim), (parts,), jnp.float32, least / len(pieces), top_value / len(pieces)))
        level = level * jnp.repeat(draws, dims[dim] // parts).reshape([-1 if axis == dim else 1 for axis in range(len(dims))])
    return level


def bell_draw(rng, shape, deviation, limit, cuts=(), held_as=jnp.bfloat16):
    drawn = jax.random.normal(rng, shape, jnp.float32) * deviation
    if len(cuts) > 0:
        drawn = block_levels(rng, shape, cuts, -0.22, 0.18) * drawn
    return jnp.clip(drawn, min=-limit, max=limit).astype(held_as)


def setup_inputs(seed: int = 0) -> dict:
    arg_keys = jax.random.split(jax.random.key(seed), 12)
    return {
        "failed_section": jax.random.randint(arg_keys[0], (REPLICAS,), 0, 1000).astype(jnp.int32),
        "token_ids": draw_token_ids(jax.random.fold_in(arg_keys[11], 71), 0),
        "section_outputs": draw_section_outputs(jax.random.fold_in(arg_keys[11], 71), 0),
        "w_query": draw_w_query(jax.random.fold_in(arg_keys[11], 71), 0),
        "w_key": draw_w_key(jax.random.fold_in(arg_keys[11], 71), 0),
        "w_value": bell_draw(arg_keys[5], (SECTIONS, D, INNER), D ** -0.5, 0.125, ((0, 4), (1, 2), (2, 4)), jnp.float32),
        "w_out": bell_draw(arg_keys[6], (SECTIONS, D, INNER), (INNER // 16) ** -0.5, 0.75, ((0, 4), (1, 2), (2, 4)), jnp.float32),
        "m_value": bell_draw(arg_keys[7], (SECTIONS, D, INNER), 0.5, 3.0, ((0, 4), (1, 2), (2, 4)), jnp.float32),
        "v_value": jnp.clip(jnp.exp(math.log(1.0) - 6.9077552 * jax.random.uniform(arg_keys[8], (SECTIONS, D, INNER), jnp.float32) ** block_levels(arg_keys[8], (SECTIONS, D, INNER), ((0, 4), (1, 2), (2, 4)), -0.2, 0.2)), 0.001, 1.0),
        "m_out": bell_draw(arg_keys[9], (SECTIONS, D, INNER), 0.5, 3.0, ((0, 4), (1, 2), (2, 4)), jnp.float32),
        "v_out": jnp.clip(jnp.exp(math.log(1.0) - 6.9077552 * jax.random.uniform(arg_keys[10], (SECTIONS, D, INNER), jnp.float32) ** block_levels(arg_keys[10], (SECTIONS, D, INNER), ((0, 4), (1, 2), (2, 4)), -0.2, 0.2)), 0.001, 1.0),
    }


end_token = 100001
mask_fill = -1e+30

def document_ids(token_row):
    doc_ends = (token_row == end_token).astype(jnp.int32)
    return jnp.cumsum(doc_ends) - doc_ends

def attend_head(query_head, key_head, value_head, allowed):
    scores = jnp.dot(query_head, key_head.T, preferred_element_type=jnp.float32) * (1.0 / math.sqrt(HD))
    scores = jnp.where(allowed, scores, mask_fill)
    highest = lax.optimization_barrier(jnp.max(scores, axis=1, keepdims=True))
    weights = jnp.exp(scores - highest)
    probs = (weights / lax.optimization_barrier(jnp.sum(weights, axis=1, keepdims=True))).astype(jnp.bfloat16)
    return jnp.dot(probs, value_head, preferred_element_type=jnp.float32).astype(jnp.bfloat16)

def recompute(incoming, token_row, query_master, key_master, value_master, out_master):
    queries = jnp.dot(incoming, query_master.astype(jnp.bfloat16), preferred_element_type=jnp.float32).astype(jnp.bfloat16)
    key_vals = jnp.dot(incoming, key_master.astype(jnp.bfloat16), preferred_element_type=jnp.float32).astype(jnp.bfloat16)
    value_vals = jnp.dot(incoming, value_master.astype(jnp.bfloat16), preferred_element_type=jnp.float32).astype(jnp.bfloat16)
    query_heads = queries.reshape(TOKENS, HEADS, HD).transpose(1, 0, 2)
    key_heads = key_vals.reshape(TOKENS, HEADS, HD).transpose(1, 0, 2)
    value_heads = value_vals.reshape(TOKENS, HEADS, HD).transpose(1, 0, 2)
    document = document_ids(token_row)
    positions = jnp.arange(TOKENS)
    allowed = (positions[None, :] <= positions[:, None]) & (document[None, :] == document[:, None])
    context = lax.map(lambda trio: attend_head(trio[0], trio[1], trio[2], allowed), (query_heads, key_heads, value_heads))
    context = context.transpose(1, 0, 2).reshape(TOKENS, INNER)
    return jnp.dot(context, out_master.astype(jnp.bfloat16).T, preferred_element_type=jnp.float32).astype(jnp.bfloat16)

def reference(failed_section, token_ids, section_outputs, w_query, w_key, w_value, w_out, m_value, v_value, m_out, v_out):
    sources = (w_query, w_key, w_value, w_out, m_value, v_value, m_out, v_out)
    results = [jnp.zeros((REPLICAS, SECTIONS, D, INNER), jnp.float32) for item in sources]
    update_all = jnp.zeros((REPLICAS, SECTIONS, TOKENS, D), jnp.bfloat16)
    for replica in range(REPLICAS):
        section_failed = jnp.remainder(failed_section[replica], SECTIONS).astype(jnp.int32)
        before = jnp.remainder(section_failed + SECTIONS - 1, SECTIONS).astype(jnp.int32)
        incoming = section_outputs[replica, before]
        blocks = [source[section_failed] for source in sources]
        update = recompute(incoming, token_ids[replica], blocks[0], blocks[1], blocks[2], blocks[3])
        results = [result.at[replica, section_failed].set(block) for result, block in zip(results, blocks)]
        update_all = update_all.at[replica, section_failed].set(update)
    return (results[0], results[1], results[2], results[3], results[4], results[5], results[6], results[7], update_all)
```

```python
import math

import jax
import jax.numpy as jnp
from jax import lax
from jax.experimental import pallas as pl
from jax.experimental.pallas import tpu as pltpu
from jax.sharding import PartitionSpec as P

HD = 128


end_token = 100001
mask_fill = -1e30


def passed_along(array, axis, by):
    count = lax.axis_size(axis)
    return lax.ppermute(array, axis, [(i, (i + by) % count) for i in range(count)])


def document_ids(token_row):
    doc_ends = (token_row == end_token).astype(jnp.int32)
    return jnp.cumsum(doc_ends) - doc_ends


def attend(queries, key_vals, value_vals, token_row):
    token_count = queries.shape[0]
    heads_local = queries.shape[1] // HD
    block_rows = min(512, token_count)
    document = document_ids(token_row)
    positions = jnp.arange(token_count, dtype=jnp.int32)
    key_heads = key_vals.reshape(token_count, heads_local, HD)
    value_heads = value_vals.reshape(token_count, heads_local, HD)

    def one_block(block_index):
        first_row = block_index * block_rows
        query_block = lax.dynamic_slice_in_dim(queries, first_row, block_rows, 0).reshape(
            block_rows, heads_local, HD
        )
        scores = jnp.einsum(
            "qhd,khd->hqk", query_block, key_heads, preferred_element_type=jnp.float32
        ) * (1.0 / math.sqrt(HD))
        query_pos = lax.dynamic_slice_in_dim(positions, first_row, block_rows, 0)
        query_doc = lax.dynamic_slice_in_dim(document, first_row, block_rows, 0)
        allowed = (positions[None, :] <= query_pos[:, None]) & (
            document[None, :] == query_doc[:, None]
        )
        scores = jnp.where(allowed[None], scores, mask_fill)
        highest = jnp.max(scores, axis=2, keepdims=True)
        weights = jnp.exp(scores - highest)
        probs = (weights / jnp.sum(weights, axis=2, keepdims=True)).astype(jnp.bfloat16)
        context = jnp.einsum(
            "hqk,khd->qhd", probs, value_heads, preferred_element_type=jnp.float32
        ).astype(jnp.bfloat16)
        return context.reshape(block_rows, heads_local * HD)

    blocks = lax.map(one_block, jnp.arange(token_count // block_rows, dtype=jnp.int32))
    return blocks.reshape(token_count, heads_local * HD)


def shards(
    failed_section,
    token_ids,
    section_outputs,
    w_query,
    w_key,
    w_value,
    w_out,
    m_value,
    v_value,
    m_out,
    v_out,
):
    section_failed = jnp.remainder(failed_section[0], lax.axis_size("section"))
    replacing = lax.axis_index("section") == section_failed
    states = (
        lax.all_gather(w_query, "dp", axis=1, tiled=True),
        lax.all_gather(w_key, "dp", axis=1, tiled=True),
        lax.all_gather(w_value, "dp", axis=1, tiled=True),
        lax.all_gather(w_out, "dp", axis=1, tiled=True),
        lax.all_gather(m_value, "dp", axis=1, tiled=True),
        lax.all_gather(v_value, "dp", axis=1, tiled=True),
        lax.all_gather(m_out, "dp", axis=1, tiled=True),
        lax.all_gather(v_out, "dp", axis=1, tiled=True),
    )
    masters = states[:4]
    moments = states[4:]
    query_bf = masters[0][0].astype(jnp.bfloat16)
    key_bf = masters[1][0].astype(jnp.bfloat16)
    value_bf = masters[2][0].astype(jnp.bfloat16)
    out_bf = masters[3][0].astype(jnp.bfloat16)
    inner_local = query_bf.shape[1]
    w_joined = jnp.concatenate([query_bf, key_bf, value_bf], axis=1)
    incoming = passed_along(section_outputs, "section", 1)
    projected = jnp.dot(
        lax.all_gather(incoming, "tensor", axis=3, tiled=True)[0, 0],
        w_joined,
        preferred_element_type=jnp.float32,
    )
    queries = projected[:, :inner_local].astype(jnp.bfloat16)
    key_vals = projected[:, inner_local : 2 * inner_local].astype(jnp.bfloat16)
    value_vals = projected[:, 2 * inner_local :].astype(jnp.bfloat16)
    context = attend(queries, key_vals, value_vals, token_ids[0])
    context_whole = lax.all_gather(context, "tensor", axis=1, tiled=True)
    out_slice = lax.all_to_all(out_bf, "tensor", split_axis=0, concat_axis=1, tiled=True)
    update = lax.dot_general(
        context_whole, out_slice, (((1,), (1,)), ((), ())), preferred_element_type=jnp.float32
    ).astype(jnp.bfloat16)

    def placed(gathered):
        return jnp.where(replacing, gathered[None], jnp.zeros_like(gathered[None]))

    update_block = jnp.where(
        replacing, update[None, None], jnp.zeros((1, 1) + update.shape, jnp.bfloat16)
    )
    return (
        placed(masters[0]),
        placed(masters[1]),
        placed(masters[2]),
        placed(masters[3]),
        placed(moments[0]),
        placed(moments[1]),
        placed(moments[2]),
        placed(moments[3]),
        update_block,
    )


def swapped(array):
    count = lax.axis_size("section")
    return lax.ppermute(array, "section", [(i, i ^ 1) for i in range(count)])


def crossed(array):
    return lax.ppermute(array, "dp", [(0, 1), (1, 0)])


def shifted(array, by):
    return passed_along(array, "tensor", by)


def attend_kernel(qkv_q, k_mine, v_mine, k_other, v_other, q_pos, q_doc, k_pos, k_doc, out):
    q = qkv_q[...]
    dims = (((1,), (1,)), ((), ()))
    scores = jnp.concatenate(
        [
            lax.dot_general(q, k_mine[...], dims, preferred_element_type=jnp.float32),
            lax.dot_general(q, k_other[...], dims, preferred_element_type=jnp.float32),
        ],
        axis=1,
    ) * (1.0 / math.sqrt(HD))
    allowed = (k_pos[...] <= q_pos[...]) & (k_doc[...] == q_doc[...])
    scores = jnp.where(allowed, scores, mask_fill)
    weights = jnp.exp(scores - jnp.max(scores, axis=1, keepdims=True))
    total = jnp.sum(weights, axis=1, keepdims=True)
    probs = weights.astype(jnp.bfloat16)
    half = k_mine.shape[0]
    context = jnp.dot(
        probs[:, :half], v_mine[...], preferred_element_type=jnp.float32
    ) + jnp.dot(probs[:, half:], v_other[...], preferred_element_type=jnp.float32)
    out[...] = (context / total).astype(jnp.bfloat16)


def attend_pair(qkv, kv_other, q_pos, q_doc, k_pos, k_doc):
    rows = qkv.shape[0]
    heads = qkv.shape[1] // (3 * HD)
    block = min(256, rows)
    keys = 2 * rows
    return pl.pallas_call(
        attend_kernel,
        grid=(heads, rows // block),
        out_shape=jax.ShapeDtypeStruct((rows, heads * HD), jnp.bfloat16),
        in_specs=[
            pl.BlockSpec((block, HD), lambda h, i: (i, h)),
            pl.BlockSpec((rows, HD), lambda h, i: (0, heads + h)),
            pl.BlockSpec((rows, HD), lambda h, i: (0, 2 * heads + h)),
            pl.BlockSpec((rows, HD), lambda h, i: (0, h)),
            pl.BlockSpec((rows, HD), lambda h, i: (0, heads + h)),
            pl.BlockSpec((block, 1), lambda h, i: (i, 0)),
            pl.BlockSpec((block, 1), lambda h, i: (i, 0)),
            pl.BlockSpec((1, keys), lambda h, i: (0, 0)),
            pl.BlockSpec((1, keys), lambda h, i: (0, 0)),
        ],
        out_specs=pl.BlockSpec((block, HD), lambda h, i: (i, h)),
        cost_estimate=pl.CostEstimate(
            flops=4 * rows * keys * heads * HD,
            bytes_accessed=10 * rows * heads * HD,
            transcendentals=rows * keys * heads,
        ),
        compiler_params=pltpu.CompilerParams(vmem_limit_bytes=40 * 2**20),
    )(qkv, qkv, qkv, kv_other, kv_other, q_pos, q_doc, k_pos, k_doc)


def shards_pair(
    failed_section,
    token_ids,
    section_outputs,
    w_query,
    w_key,
    w_value,
    w_out,
    m_value,
    v_value,
    m_out,
    v_out,
):
    sections = lax.axis_size("section")
    ranks = lax.axis_size("tensor")
    section = lax.axis_index("section")
    core = section % 2
    replica = lax.axis_index("dp")
    rank = lax.axis_index("tensor")
    failed = jnp.remainder(failed_section[0], sections)
    failed_peer = crossed(failed[None])[0]
    replacing = section == failed
    failed_here = (failed % 2) == core

    acts = section_outputs[0, 0]
    tokens = acts.shape[0]
    half_tokens = tokens // 2
    half0, half1 = acts[:half_tokens], acts[half_tokens:]
    from_last = passed_along(jnp.where(core == 1, half0, half1), "section", 1)
    from_far = lax.ppermute(
        half1, "section", [(i, (i + 2) % sections) for i in range(sections) if i % 2 == 1]
    )
    from_even = jnp.where(core == 0, from_last, from_far)
    from_odd = jnp.where(core == 0, half0, from_last)
    incoming = jnp.where((failed % 2) == 0, from_even, from_odd)

    def half_of(array, index):
        rows = array.shape[0] // 2
        return lax.dynamic_slice_in_dim(array, index * rows, rows, 0)

    def fetched(array):
        own = array[0]
        theirs = swapped(half_of(own, 1 - core))
        sent = jnp.where(failed_peer == section, half_of(own, core), theirs)
        got = crossed(sent)
        return own, got, swapped(got)

    def block_list(own, got, other):
        rows = got.shape[0]
        halves = (own[:rows], own[rows:])
        return [
            jnp.where(
                replica == b // 2, halves[b % 2], jnp.where(core == b % 2, got, other)
            )
            for b in range(4)
        ]

    masters = [fetched(w) for w in (w_query, w_key, w_value, w_out)]
    moments = [fetched(m) for m in (m_value, v_value, m_out, v_out)]

    def in_bf(trio):
        own, got, other = trio
        own_bf = own.astype(jnp.bfloat16)
        own_bf = jnp.where(failed_here, own_bf, swapped(own_bf))
        return block_list(own_bf, got.astype(jnp.bfloat16), other.astype(jnp.bfloat16))

    qkv_blocks = [in_bf(trio) for trio in masters[:3]]
    weight = jnp.concatenate(
        [jnp.concatenate(blocks, axis=0) for blocks in qkv_blocks], axis=1
    )
    out_weight = jnp.concatenate(in_bf(masters[3]), axis=0)

    width = incoming.shape[1]
    projected = None
    for by in range(ranks):
        chunk = incoming if by == 0 else shifted(incoming, by)
        owner = (rank - by) % ranks
        part = jnp.dot(
            chunk,
            lax.dynamic_slice_in_dim(weight, owner * width, width, 0),
            preferred_element_type=jnp.float32,
        )
        projected = part if projected is None else projected + part
    qkv = projected.astype(jnp.bfloat16)
    inner = qkv.shape[1] // 3
    kv_other = swapped(qkv[:, inner:])

    document = document_ids(token_ids[0])
    positions = jnp.arange(tokens, dtype=jnp.int32)
    doc_mine, doc_other = half_of(document, core), half_of(document, 1 - core)
    pos_mine, pos_other = half_of(positions, core), half_of(positions, 1 - core)
    context = attend_pair(
        qkv,
        kv_other,
        pos_mine[:, None],
        doc_mine[:, None],
        jnp.concatenate([pos_mine, pos_other])[None],
        jnp.concatenate([doc_mine, doc_other])[None],
    )

    out_width = out_weight.shape[0] // ranks
    update = None
    for by in range(ranks):
        target = (rank + by) % ranks
        rows = lax.dynamic_slice_in_dim(out_weight, target * out_width, out_width, 0)
        chunk = context
        if by > 0:
            rows, chunk = shifted(rows, by), shifted(context, by)
        part = lax.dot_general(
            chunk, rows, (((1,), (1,)), ((), ())), preferred_element_type=jnp.float32
        )
        update = part if update is None else update + part
    update = update.astype(jnp.bfloat16)
    update_other = swapped(update)
    update_whole = jnp.concatenate(
        [
            jnp.where(core == 0, update, update_other),
            jnp.where(core == 0, update_other, update),
        ],
        axis=0,
    )
    update_block = jnp.where(replacing, update_whole, jnp.zeros_like(update_whole))[None, None]

    def placed(trio):
        blocks = jnp.concatenate(block_list(*trio), axis=0)
        return jnp.where(replacing, blocks, jnp.zeros_like(blocks))[None, None]

    return tuple(placed(trio) for trio in masters + moments) + (update_block,)


def solution(mesh):
    paired = mesh.shape["dp"] == 2 and mesh.shape["section"] % 2 == 0 and mesh.shape["tensor"] == 4
    return jax.shard_map(
        shards_pair if paired else shards,
        mesh=mesh,
        in_specs=(
            P("dp"),
            P("dp", None),
            P("dp", "section", None, "tensor"),
            P("section", "dp", "tensor"),
            P("section", "dp", "tensor"),
            P("section", "dp", "tensor"),
            P("section", "dp", "tensor"),
            P("section", "dp", "tensor"),
            P("section", "dp", "tensor"),
            P("section", "dp", "tensor"),
            P("section", "dp", "tensor"),
        ),
        out_specs=(
            P("dp", "section", None, "tensor"),
            P("dp", "section", None, "tensor"),
            P("dp", "section", None, "tensor"),
            P("dp", "section", None, "tensor"),
            P("dp", "section", None, "tensor"),
            P("dp", "section", None, "tensor"),
            P("dp", "section", None, "tensor"),
            P("dp", "section", None, "tensor"),
            P("dp", "section", None, "tensor"),
        ),
        check_vma=False,
    )
```

```python
import math

import jax
import jax.numpy as jnp
from jax import lax
from jax.experimental import pallas as pl
from jax.experimental.pallas import tpu as pltpu
from jax.sharding import PartitionSpec as P

HD = 128


end_token = 100001
mask_fill = -1e30


def passed_along(array, axis, by):
    count = lax.axis_size(axis)
    return lax.ppermute(array, axis, [(i, (i + by) % count) for i in range(count)])


def document_ids(token_row):
    doc_ends = (token_row == end_token).astype(jnp.int32)
    return jnp.cumsum(doc_ends) - doc_ends


def attend(queries, key_vals, value_vals, token_row):
    token_count = queries.shape[0]
    heads_local = queries.shape[1] // HD
    block_rows = min(512, token_count)
    document = document_ids(token_row)
    positions = jnp.arange(token_count, dtype=jnp.int32)
    key_heads = key_vals.reshape(token_count, heads_local, HD)
    value_heads = value_vals.reshape(token_count, heads_local, HD)

    def one_block(block_index):
        first_row = block_index * block_rows
        query_block = lax.dynamic_slice_in_dim(queries, first_row, block_rows, 0).reshape(
            block_rows, heads_local, HD
        )
        scores = jnp.einsum(
            "qhd,khd->hqk", query_block, key_heads, preferred_element_type=jnp.float32
        ) * (1.0 / math.sqrt(HD))
        query_pos = lax.dynamic_slice_in_dim(positions, first_row, block_rows, 0)
        query_doc = lax.dynamic_slice_in_dim(document, first_row, block_rows, 0)
        allowed = (positions[None, :] <= query_pos[:, None]) & (
            document[None, :] == query_doc[:, None]
        )
        scores = jnp.where(allowed[None], scores, mask_fill)
        highest = jnp.max(scores, axis=2, keepdims=True)
        weights = jnp.exp(scores - highest)
        probs = (weights / jnp.sum(weights, axis=2, keepdims=True)).astype(jnp.bfloat16)
        context = jnp.einsum(
            "hqk,khd->qhd", probs, value_heads, preferred_element_type=jnp.float32
        ).astype(jnp.bfloat16)
        return context.reshape(block_rows, heads_local * HD)

    blocks = lax.map(one_block, jnp.arange(token_count // block_rows, dtype=jnp.int32))
    return blocks.reshape(token_count, heads_local * HD)


def shards(
    failed_section,
    token_ids,
    section_outputs,
    w_query,
    w_key,
    w_value,
    w_out,
    m_value,
    v_value,
    m_out,
    v_out,
):
    section_failed = jnp.remainder(failed_section[0], lax.axis_size("section"))
    replacing = lax.axis_index("section") == section_failed
    states = (
        lax.all_gather(w_query, "dp", axis=1, tiled=True),
        lax.all_gather(w_key, "dp", axis=1, tiled=True),
        lax.all_gather(w_value, "dp", axis=1, tiled=True),
        lax.all_gather(w_out, "dp", axis=1, tiled=True),
        lax.all_gather(m_value, "dp", axis=1, tiled=True),
        lax.all_gather(v_value, "dp", axis=1, tiled=True),
        lax.all_gather(m_out, "dp", axis=1, tiled=True),
        lax.all_gather(v_out, "dp", axis=1, tiled=True),
    )
    masters = states[:4]
    moments = states[4:]
    query_bf = masters[0][0].astype(jnp.bfloat16)
    key_bf = masters[1][0].astype(jnp.bfloat16)
    value_bf = masters[2][0].astype(jnp.bfloat16)
    out_bf = masters[3][0].astype(jnp.bfloat16)
    inner_local = query_bf.shape[1]
    w_joined = jnp.concatenate([query_bf, key_bf, value_bf], axis=1)
    incoming = passed_along(section_outputs, "section", 1)
    projected = jnp.dot(
        lax.all_gather(incoming, "tensor", axis=3, tiled=True)[0, 0],
        w_joined,
        preferred_element_type=jnp.float32,
    )
    queries = projected[:, :inner_local].astype(jnp.bfloat16)
    key_vals = projected[:, inner_local : 2 * inner_local].astype(jnp.bfloat16)
    value_vals = projected[:, 2 * inner_local :].astype(jnp.bfloat16)
    context = attend(queries, key_vals, value_vals, token_ids[0])
    context_whole = lax.all_gather(context, "tensor", axis=1, tiled=True)
    out_slice = lax.all_to_all(out_bf, "tensor", split_axis=0, concat_axis=1, tiled=True)
    update = lax.dot_general(
        context_whole, out_slice, (((1,), (1,)), ((), ())), preferred_element_type=jnp.float32
    ).astype(jnp.bfloat16)

    def placed(gathered):
        return jnp.where(replacing, gathered[None], jnp.zeros_like(gathered[None]))

    update_block = jnp.where(
        replacing, update[None, None], jnp.zeros((1, 1) + update.shape, jnp.bfloat16)
    )
    return (
        placed(masters[0]),
        placed(masters[1]),
        placed(masters[2]),
        placed(masters[3]),
        placed(moments[0]),
        placed(moments[1]),
        placed(moments[2]),
        placed(moments[3]),
        update_block,
    )


def swapped(array):
    count = lax.axis_size("section")
    return lax.ppermute(array, "section", [(i, i ^ 1) for i in range(count)])


def crossed(array):
    return lax.ppermute(array, "dp", [(0, 1), (1, 0)])


def shifted(array, by):
    return passed_along(array, "tensor", by)


def attend_kernel(qkv_q, k_mine, v_mine, k_other, v_other, q_pos, q_doc, k_pos, k_doc, out):
    q = qkv_q[...]
    dims = (((1,), (1,)), ((), ()))
    scores = jnp.concatenate(
        [
            lax.dot_general(q, k_mine[...], dims, preferred_element_type=jnp.float32),
            lax.dot_general(q, k_other[...], dims, preferred_element_type=jnp.float32),
        ],
        axis=1,
    ) * (1.0 / math.sqrt(HD))
    allowed = (k_pos[...] <= q_pos[...]) & (k_doc[...] == q_doc[...])
    scores = jnp.where(allowed, scores, mask_fill)
    weights = jnp.exp(scores - jnp.max(scores, axis=1, keepdims=True))
    total = jnp.sum(weights, axis=1, keepdims=True)
    probs = weights.astype(jnp.bfloat16)
    half = k_mine.shape[0]
    context = jnp.dot(
        probs[:, :half], v_mine[...], preferred_element_type=jnp.float32
    ) + jnp.dot(probs[:, half:], v_other[...], preferred_element_type=jnp.float32)
    out[...] = (context / total).astype(jnp.bfloat16)


def attend_pair(qkv, kv_other, q_pos, q_doc, k_pos, k_doc):
    rows = qkv.shape[0]
    heads = qkv.shape[1] // (3 * HD)
    block = min(256, rows)
    keys = 2 * rows
    return pl.pallas_call(
        attend_kernel,
        grid=(heads, rows // block),
        out_shape=jax.ShapeDtypeStruct((rows, heads * HD), jnp.bfloat16),
        in_specs=[
            pl.BlockSpec((block, HD), lambda h, i: (i, h)),
            pl.BlockSpec((rows, HD), lambda h, i: (0, heads + h)),
            pl.BlockSpec((rows, HD), lambda h, i: (0, 2 * heads + h)),
            pl.BlockSpec((rows, HD), lambda h, i: (0, h)),
            pl.BlockSpec((rows, HD), lambda h, i: (0, heads + h)),
            pl.BlockSpec((block, 1), lambda h, i: (i, 0)),
            pl.BlockSpec((block, 1), lambda h, i: (i, 0)),
            pl.BlockSpec((1, keys), lambda h, i: (0, 0)),
            pl.BlockSpec((1, keys), lambda h, i: (0, 0)),
        ],
        out_specs=pl.BlockSpec((block, HD), lambda h, i: (i, h)),
        cost_estimate=pl.CostEstimate(
            flops=4 * rows * keys * heads * HD,
            bytes_accessed=10 * rows * heads * HD,
            transcendentals=rows * keys * heads,
        ),
        compiler_params=pltpu.CompilerParams(vmem_limit_bytes=40 * 2**20),
    )(qkv, qkv, qkv, kv_other, kv_other, q_pos, q_doc, k_pos, k_doc)


def shards_pair(
    failed_section,
    token_ids,
    section_outputs,
    w_query,
    w_key,
    w_value,
    w_out,
    m_value,
    v_value,
    m_out,
    v_out,
):
    sections = lax.axis_size("section")
    ranks = lax.axis_size("tensor")
    section = lax.axis_index("section")
    core = section % 2
    replica = lax.axis_index("dp")
    rank = lax.axis_index("tensor")
    failed = jnp.remainder(failed_section[0], sections)
    failed_peer = crossed(failed[None])[0]
    replacing = section == failed
    failed_here = (failed % 2) == core

    acts = section_outputs[0, 0]
    tokens = acts.shape[0]
    half_tokens = tokens // 2
    half0, half1 = acts[:half_tokens], acts[half_tokens:]
    from_last = passed_along(jnp.where(core == 1, half0, half1), "section", 1)
    from_far = lax.ppermute(
        half1, "section", [(i, (i + 2) % sections) for i in range(sections) if i % 2 == 1]
    )
    from_even = jnp.where(core == 0, from_last, from_far)
    from_odd = jnp.where(core == 0, half0, from_last)
    incoming = jnp.where((failed % 2) == 0, from_even, from_odd)

    def half_of(array, index):
        rows = array.shape[0] // 2
        return lax.dynamic_slice_in_dim(array, index * rows, rows, 0)

    def fetched(array, after=None):
        own = array[0]
        theirs = swapped(half_of(own, 1 - core))
        sent = jnp.where(failed_peer == section, half_of(own, core), theirs)
        if after is not None:
            sent = lax.optimization_barrier((sent, after))[0]
        got = crossed(sent)
        return own, got, swapped(got)

    def block_list(own, got, other):
        rows = got.shape[0]
        halves = (own[:rows], own[rows:])
        return [
            jnp.where(
                replica == b // 2, halves[b % 2], jnp.where(core == b % 2, got, other)
            )
            for b in range(4)
        ]

    masters = [fetched(w) for w in (w_query, w_key, w_value)] + [fetched(w_out, incoming)]
    moments = [fetched(m, incoming) for m in (m_value, v_value, m_out, v_out)]

    def in_bf(trio):
        own, got, other = trio
        own_bf = own.astype(jnp.bfloat16)
        own_bf = jnp.where(failed_here, own_bf, swapped(own_bf))
        return block_list(own_bf, got.astype(jnp.bfloat16), other.astype(jnp.bfloat16))

    qkv_blocks = [in_bf(trio) for trio in masters[:3]]
    weight = jnp.concatenate(
        [jnp.concatenate(blocks, axis=0) for blocks in qkv_blocks], axis=1
    )
    out_weight = jnp.concatenate(in_bf(masters[3]), axis=0)

    width = incoming.shape[1]
    projected = None
    for by in range(ranks):
        chunk = incoming if by == 0 else shifted(incoming, by)
        owner = (rank - by) % ranks
        part = jnp.dot(
            chunk,
            lax.dynamic_slice_in_dim(weight, owner * width, width, 0),
            preferred_element_type=jnp.float32,
        )
        projected = part if projected is None else projected + part
    qkv = projected.astype(jnp.bfloat16)
    inner = qkv.shape[1] // 3
    kv_other = swapped(qkv[:, inner:])

    document = document_ids(token_ids[0])
    positions = jnp.arange(tokens, dtype=jnp.int32)
    doc_mine, doc_other = half_of(document, core), half_of(document, 1 - core)
    pos_mine, pos_other = half_of(positions, core), half_of(positions, 1 - core)
    context = attend_pair(
        qkv,
        kv_other,
        pos_mine[:, None],
        doc_mine[:, None],
        jnp.concatenate([pos_mine, pos_other])[None],
        jnp.concatenate([doc_mine, doc_other])[None],
    )

    out_width = out_weight.shape[0] // ranks
    update = None
    for by in range(ranks):
        target = (rank + by) % ranks
        rows = lax.dynamic_slice_in_dim(out_weight, target * out_width, out_width, 0)
        chunk = context
        if by > 0:
            rows, chunk = shifted(rows, by), shifted(context, by)
        part = lax.dot_general(
            chunk, rows, (((1,), (1,)), ((), ())), preferred_element_type=jnp.float32
        )
        update = part if update is None else update + part
    update = update.astype(jnp.bfloat16)
    update_other = swapped(update)
    update_whole = jnp.concatenate(
        [
            jnp.where(core == 0, update, update_other),
            jnp.where(core == 0, update_other, update),
        ],
        axis=0,
    )
    update_block = jnp.where(replacing, update_whole, jnp.zeros_like(update_whole))[None, None]

    def placed(trio):
        blocks = jnp.concatenate(block_list(*trio), axis=0)
        return jnp.where(replacing, blocks, jnp.zeros_like(blocks))[None, None]

    return tuple(placed(trio) for trio in masters + moments) + (update_block,)


def solution(mesh):
    paired = mesh.shape["dp"] == 2 and mesh.shape["section"] % 2 == 0 and mesh.shape["tensor"] == 4
    return jax.shard_map(
        shards_pair if paired else shards,
        mesh=mesh,
        in_specs=(
            P("dp"),
            P("dp", None),
            P("dp", "section", None, "tensor"),
            P("section", "dp", "tensor"),
            P("section", "dp", "tensor"),
            P("section", "dp", "tensor"),
            P("section", "dp", "tensor"),
            P("section", "dp", "tensor"),
            P("section", "dp", "tensor"),
            P("section", "dp", "tensor"),
            P("section", "dp", "tensor"),
        ),
        out_specs=(
            P("dp", "section", None, "tensor"),
            P("dp", "section", None, "tensor"),
            P("dp", "section", None, "tensor"),
            P("dp", "section", None, "tensor"),
            P("dp", "section", None, "tensor"),
            P("dp", "section", None, "tensor"),
            P("dp", "section", None, "tensor"),
            P("dp", "section", None, "tensor"),
            P("dp", "section", None, "tensor"),
        ),
        check_vma=False,
    )
```
